32 devices in a mesh: seq: 16 (over z, y, core), head: 2 (over x).
Axes of the slice: x: 2, y: 2, z: 4, core: 2. Of those that a mesh axis runs over, the one named last changes fastest.
Arguments:
- tokens: bfloat16 [8192, 2048], P('seq', 'head'), may hold values from -200 to 200
- norm_gain: float32 [2, 2048], replicated, may hold values from 0.25 to 1.75
- w_query: bfloat16 [2, 2048, 2048], P(None, None, 'head'), may hold values from -0.35 to 0.35
- key_projection_weight: bfloat16 [2, 2048, 512], P(None, None, 'head'), may hold values from -0.35 to 0.35
- value_projection_weight: bfloat16 [2, 2048, 512], P(None, None, 'head'), may hold values from -0.125 to 0.125
- w_out: bfloat16 [2, 2048, 2048], P(None, 'head'), may hold values from -0.125 to 0.125
- counts: int32 [16], replicated, may hold values from 128 to 512
Outputs:
- hidden_out: bfloat16 [8192, 2048], P('seq', 'head')
The draws below stay inside these ranges and needn't reach their ends.
Inputs may be any that keep to these rules, and one draw needn't show every extreme that they name: The first counts[b] tokens of block b of 512 positions are valid keys; the rest of the block is padding that no query uses as a key.
All inputs are finite; a program needn't handle non-finite values.
Results may differ from the reference program's by a relative error of at most 0.02.
The reference program's roundings to bfloat16 on the way count: a program that leaves them out, or rounds other values in their place, can miss the bound.
Values may be sent and summed in bfloat16 or wider, within the bound.
No kernel may reach another device: no remote copies, remote signals or barrier semaphores. Data moves between devices by JAX's collectives and lax.ppermute only.
A program may use at most 128 MiB of HBM per device.

```python
import math
import jax
import jax.numpy as jnp
from jax import lax

MODEL_WIDTH = 2048
QUERY_HEAD_COUNT = 16
KEY_VALUE_HEADS = 4
HEAD_SIZE = 128
WINDOW = 4096
LAYER_COUNT = 2
BLOCK_TOKENS = 512
BLOCKS = 16
SEQUENCE_TOKENS = 8192
N_HEAD = 2


def sample_projection(key, salt, columns):
    scale_value = 1.6 / math.sqrt(MODEL_WIDTH)
    inner = jax.random.fold_in(key, salt)
    sampled_values = scale_value * jax.random.normal(inner, (LAYER_COUNT, MODEL_WIDTH, columns), jnp.float32)
    return jnp.clip(sampled_values, -0.35, 0.35)


def draw_w_query(key, part):
    sampled_values = sample_projection(key, 101, QUERY_HEAD_COUNT * HEAD_SIZE)
    return sampled_values.astype(jnp.bfloat16)


def draw_key_projection_weight(key, part):
    sampled_values = sample_projection(key, 102, KEY_VALUE_HEADS * HEAD_SIZE)
    return sampled_values.astype(jnp.bfloat16)


def draw_tokens(key, part):
    inner = jax.random.fold_in(key, 201)
    values = jnp.clip(jax.random.normal(inner, (SEQUENCE_TOKENS, MODEL_WIDTH), jnp.float32), -6.0, 6.0)
    return values.astype(jnp.bfloat16)


def set_ends(entries, rng, smallest, top_value):
    index_at = [jax.random.randint(jax.random.fold_in(rng, axis), (), 0, length) for axis, length in enumerate(entries.shape)]
    longest = entries.shape.index(max(entries.shape))
    next_to = index_at[:longest] + [(index_at[longest] + 1) % entries.shape[longest]] + index_at[longest + 1:]
    return entries.at[tuple(index_at)].set(smallest).at[tuple(next_to)].set(top_value)


def levels(key, dims, pieces, smallest, top_value):
    factor_of, own = 1.0, jax.random.fold_in(key, 6)
    for dim, shards_of in pieces:
        steps = jnp.exp(jax.random.uniform(jax.random.fold_in(own, dim), (shards_of,), jnp.float32, smallest / len(pieces), top_value / len(pieces)))
        factor_of = factor_of * jnp.repeat(steps, dims[dim] // shards_of).reshape([-1 if axis == dim else 1 for axis in range(len(dims))])
    return factor_of


def normal_values(stream_key, dims, width, most, pieces=(), kind=jnp.bfloat16):
    result = width * jax.random.normal(stream_key, dims, jnp.float32)
    if pieces:
        result = result * levels(stream_key, dims, pieces, -0.22, 0.18)
    return jnp.clip(result, -most, most).astype(kind)


def setup_inputs(seed: int = 0) -> dict:
    keys = jax.random.split(jax.random.key(seed), 8)
    return {
        "tokens": draw_tokens(jax.random.fold_in(keys[7], 71), 0),
        "norm_gain": jnp.clip(1.0 + 0.15 * jax.random.normal(keys[1], (LAYER_COUNT, MODEL_WIDTH), jnp.float32), 0.25, 1.75),
        "w_query": draw_w_query(jax.random.fold_in(keys[7], 71), 0),
        "key_projection_weight": draw_key_projection_weight(jax.random.fold_in(keys[7], 71), 0),
        "value_projection_weight": normal_values(keys[4], (LAYER_COUNT, MODEL_WIDTH, KEY_VALUE_HEADS * HEAD_SIZE), MODEL_WIDTH ** -0.5, 0.125, ((2, 2),)),
        "w_out": normal_values(keys[5], (LAYER_COUNT, QUERY_HEAD_COUNT * HEAD_SIZE, MODEL_WIDTH), (QUERY_HEAD_COUNT * HEAD_SIZE) ** -0.5, 0.125, ((1, 2),)),
        "counts": set_ends(jax.random.randint(keys[6], (BLOCKS,), BLOCK_TOKENS // 4, BLOCK_TOKENS + 1), jax.random.fold_in(keys[6], 1), BLOCK_TOKENS // 4, BLOCK_TOKENS).astype(jnp.int32),
    }


norm_epsilon = 1e-05
rope_base = 10000.0

def rms_norm(hidden, gain_row):
    widened = hidden.astype(jnp.float32)
    mean_square = lax.optimization_barrier(jnp.mean(widened * widened, axis=-1, keepdims=True))
    scaled = widened * lax.rsqrt(mean_square + norm_epsilon) * gain_row.astype(jnp.float32)
    return scaled.astype(jnp.bfloat16)

def apply_rotary_embedding(projected, token_positions, head_count):
    row_total = projected.shape[0]
    shaped = projected.reshape(row_total, head_count, HEAD_SIZE)
    half_dim = HEAD_SIZE // 2
    inverse = jnp.power(jnp.float32(rope_base), -2.0 * jnp.arange(half_dim, dtype=jnp.float32) / HEAD_SIZE)
    angles = token_positions.astype(jnp.float32)[:, None] * inverse[None, :]
    cosine_table = jnp.cos(angles)[:, None, :]
    sine_table = jnp.sin(angles)[:, None, :]
    first_half = shaped[..., :half_dim]
    second_half = shaped[..., half_dim:]
    rotated = jnp.concatenate([first_half * cosine_table - second_half * sine_table, second_half * cosine_table + first_half * sine_table], axis=-1)
    return rotated.astype(jnp.bfloat16)

def key_validity(key_positions, counts):
    key_block = jnp.floor_divide(key_positions, BLOCK_TOKENS)
    within_block = key_positions - key_block * BLOCK_TOKENS
    block_count = counts[jnp.clip(key_block, 0, BLOCKS - 1)]
    return (key_positions >= 0) & (within_block < block_count)

def attend(queries, key_rows_full, value_rows_full, counts):
    span_blocks = WINDOW // BLOCK_TOKENS
    group_length = QUERY_HEAD_COUNT // KEY_VALUE_HEADS
    padding_rows = span_blocks * BLOCK_TOKENS
    key_rows_padded = jnp.concatenate([jnp.zeros((padding_rows, KEY_VALUE_HEADS, HEAD_SIZE), jnp.bfloat16), key_rows_full], axis=0)
    value_rows_padded = jnp.concatenate([jnp.zeros((padding_rows, KEY_VALUE_HEADS, HEAD_SIZE), jnp.bfloat16), value_rows_full], axis=0)
    key_length = (span_blocks + 1) * BLOCK_TOKENS
    scale_factor = 1.0 / math.sqrt(HEAD_SIZE)

    def one_block(block_index):
        first_row = block_index * BLOCK_TOKENS
        block_of_queries = lax.dynamic_slice_in_dim(queries, first_row, BLOCK_TOKENS, 0)
        key_block = lax.dynamic_slice_in_dim(key_rows_padded, first_row, key_length, 0)
        value_block = lax.dynamic_slice_in_dim(value_rows_padded, first_row, key_length, 0)
        query_positions = first_row + jnp.arange(BLOCK_TOKENS, dtype=jnp.int32)
        key_positions = first_row - padding_rows + jnp.arange(key_length, dtype=jnp.int32)
        allowed = key_validity(key_positions, counts)[None, :]
        allowed = allowed & (key_positions[None, :] <= query_positions[:, None])
        allowed = allowed & (query_positions[:, None] - key_positions[None, :] < WINDOW)
        query_broad = block_of_queries.astype(jnp.float32).reshape(BLOCK_TOKENS, KEY_VALUE_HEADS, group_length, HEAD_SIZE)
        key_wide = key_block.astype(jnp.float32)
        scores = jnp.einsum('tkgd,lkd->kgtl', query_broad, key_wide, precision=lax.Precision.HIGHEST) * scale_factor
        scores = jnp.where(allowed[None, None], scores, -jnp.inf)
        largest = lax.optimization_barrier(jnp.max(scores, axis=-1, keepdims=True))
        weights = jnp.exp(scores - largest)
        weights = (weights / lax.optimization_barrier(jnp.sum(weights, axis=-1, keepdims=True))).astype(jnp.bfloat16)
        blended = jnp.einsum('kgtl,lkd->tkgd', weights.astype(jnp.float32), value_block.astype(jnp.float32), precision=lax.Precision.HIGHEST)
        return blended.astype(jnp.bfloat16).reshape(BLOCK_TOKENS, QUERY_HEAD_COUNT * HEAD_SIZE)
    outputs = lax.map(one_block, jnp.arange(BLOCKS, dtype=jnp.int32))
    return outputs.reshape(BLOCKS * BLOCK_TOKENS, QUERY_HEAD_COUNT * HEAD_SIZE)

def reference(tokens, norm_gain, w_query, key_projection_weight, value_projection_weight, w_out, counts):
    hidden = tokens
    token_positions = jnp.arange(SEQUENCE_TOKENS, dtype=jnp.int32)
    group_width = QUERY_HEAD_COUNT * HEAD_SIZE // N_HEAD
    for layer_position in range(LAYER_COUNT):
        normalized_rows = rms_norm(hidden, norm_gain[layer_position])
        queries = apply_rotary_embedding(jnp.dot(normalized_rows, w_query[layer_position], preferred_element_type=jnp.float32), token_positions, QUERY_HEAD_COUNT)
        key_rows_full = apply_rotary_embedding(jnp.dot(normalized_rows, key_projection_weight[layer_position], preferred_element_type=jnp.float32), token_positions, KEY_VALUE_HEADS)
        value_rows_full = jnp.dot(normalized_rows, value_projection_weight[layer_position], preferred_element_type=jnp.float32).astype(jnp.bfloat16).reshape(SEQUENCE_TOKENS, KEY_VALUE_HEADS, HEAD_SIZE)
        attended = attend(queries, key_rows_full, value_rows_full, counts)
        branch = jnp.zeros((SEQUENCE_TOKENS, MODEL_WIDTH), jnp.float32)
        for group_index in range(N_HEAD):
            column_start = group_index * group_width
            partial_product = jnp.dot(attended[:, column_start:column_start + group_width], w_out[layer_position, column_start:column_start + group_width], preferred_element_type=jnp.float32)
            rounded = lax.optimization_barrier(partial_product.astype(jnp.bfloat16))
            branch = branch + rounded.astype(jnp.float32)
        hidden = (hidden.astype(jnp.float32) + branch).astype(jnp.bfloat16)
    return hidden
```

```python
import functools
import math

import jax
import jax.numpy as jnp
from jax import lax
from jax.experimental import pallas as pl
from jax.experimental.pallas import tpu as pltpu
from jax.sharding import PartitionSpec as P

HEAD_SIZE = 128
WINDOW = 4096
norm_epsilon = 1e-05
rope_base = 10000.0
NEG = -1e30
TILE = 256
BF = jnp.bfloat16
F32 = jnp.float32


def _dot(a, b):
    return jnp.dot(a, b, preferred_element_type=F32)


def _dot_nt(a, b):
    return lax.dot_general(a, b, (((1,), (1,)), ((), ())), preferred_element_type=F32)


def _kv_kernel(
    sc, own, oth, g_own, g_oth, wk_own, wk_oth, wv_own, wv_oth, cos, sin, pay, n_own, n_oth, row0
):
    step = pl.program_id(0)
    a = own[...].astype(F32)
    b = oth[...].astype(F32)
    width = a.shape[1] + b.shape[1]
    total = jnp.sum(a * a, axis=1, keepdims=True) + jnp.sum(b * b, axis=1, keepdims=True)
    r = lax.rsqrt(total * (1.0 / width) + norm_epsilon)
    na = (a * r * g_own[...]).astype(BF)
    nb = (b * r * g_oth[...]).astype(BF)
    n_own[...] = na
    n_oth[...] = nb
    k = _dot(na, wk_own[...]) + _dot(nb, wk_oth[...])
    v = _dot(na, wv_own[...]) + _dot(nb, wv_oth[...])
    c = cos[...]
    s = sin[...]
    rows = a.shape[0]
    parts = []
    for h in range(k.shape[1] // HEAD_SIZE):
        x = k[:, h * HEAD_SIZE : (h + 1) * HEAD_SIZE]
        parts.append(x * c + pltpu.roll(x, HEAD_SIZE // 2, 1) * s)
    k = jnp.concatenate(parts, axis=1)

    @pl.when(step == 0)
    def _():
        row0[...] = k[0:8, :]

    valid = (step * rows + lax.broadcasted_iota(jnp.int32, k.shape, 0)) < sc[1]
    pay[0] = jnp.where(valid, k, row0[0:1, :]).astype(BF)
    pay[1] = jnp.transpose(jnp.where(valid, v, 0.0)).astype(BF)


def kv_project(layer, scal, own, oth, gain, wk, wv, cos, sin):
    rows, half = own.shape
    width = wk.shape[2]
    spec = pl.BlockSpec
    half_rows = spec((TILE, half), lambda r, sc: (r, 0))
    table = spec((TILE, HEAD_SIZE), lambda r, sc: (r, 0))
    w_own = spec((None, half, width), lambda r, sc: (layer, sc[0], 0))
    w_oth = spec((None, half, width), lambda r, sc: (layer, 1 - sc[0], 0))
    gain4 = gain.reshape(gain.shape[0], 2, 1, half)
    ga = spec((None, None, 1, half), lambda r, sc: (layer, sc[0], 0, 0))
    gb = spec((None, None, 1, half), lambda r, sc: (layer, 1 - sc[0], 0, 0))
    steps = rows // TILE
    return pl.pallas_call(
        _kv_kernel,
        grid_spec=pltpu.PrefetchScalarGridSpec(
            num_scalar_prefetch=1,
            grid=(steps,),
            in_specs=[half_rows, half_rows, ga, gb, w_own, w_oth, w_own, w_oth, table, table],
            out_specs=[
                spec((None, 2, TILE, TILE), lambda r, sc: (r, 0, 0, 0)),
                half_rows,
                half_rows,
            ],
            scratch_shapes=[pltpu.VMEM((8, width), F32)],
        ),
        out_shape=[
            jax.ShapeDtypeStruct((steps, 2, TILE, width), BF),
            jax.ShapeDtypeStruct((rows, half), BF),
            jax.ShapeDtypeStruct((rows, half), BF),
        ],
        compiler_params=pltpu.CompilerParams(dimension_semantics=("arbitrary",)),
        name="kv_project",
    )(scal, own, oth, gain4, gain4, wk, wk, wv, wv, cos, sin)


def _q_kernel(sc, na, nb, w_own, w_oth, cos, sin, out):
    q = _dot(na[...], w_own[...]) + _dot(nb[...], w_oth[...])
    c = cos[...]
    s = sin[...]
    factor = math.log2(math.e) / math.sqrt(HEAD_SIZE)
    for h in range(q.shape[1] // HEAD_SIZE):
        x = q[:, h * HEAD_SIZE : (h + 1) * HEAD_SIZE]
        y = (x * c + pltpu.roll(x, HEAD_SIZE // 2, 1) * s) * factor
        out[:, h * HEAD_SIZE : (h + 1) * HEAD_SIZE] = y.astype(BF)


def q_project(layer, scal, na, nb, wq, cos, sin):
    rows, half = na.shape
    width = wq.shape[2]
    cols = 256
    spec = pl.BlockSpec
    full = spec((rows, half), lambda j, sc: (0, 0))
    table = spec((rows, HEAD_SIZE), lambda j, sc: (0, 0))
    return pl.pallas_call(
        _q_kernel,
        grid_spec=pltpu.PrefetchScalarGridSpec(
            num_scalar_prefetch=1,
            grid=(width // cols,),
            in_specs=[
                full,
                full,
                spec((None, half, cols), lambda j, sc: (layer, sc[0], j)),
                spec((None, half, cols), lambda j, sc: (layer, 1 - sc[0], j)),
                table,
                table,
            ],
            out_specs=spec((rows, cols), lambda j, sc: (0, j)),
        ),
        out_shape=jax.ShapeDtypeStruct((rows, width), BF),
        compiler_params=pltpu.CompilerParams(dimension_semantics=("arbitrary",)),
        name="q_project",
    )(scal, na, nb, wq, wq, cos, sin)


def _attn_kernel(sc, q_ref, *refs, arrays, heads, tiles):
    kv = refs[:arrays]
    out, buf, ones, m_ref, acc_ref, sems = refs[arrays:]
    g = pl.program_id(0)
    interior = sc[arrays]
    has_edge = sc[arrays + 1]
    cbase = arrays + 2

    def wait(slot):
        pltpu.make_async_copy(kv[0], buf.at[slot], sems.at[slot]).wait()
        cnt = sc[cbase + slot]
        for r in range(tiles):
            idx = r * TILE + lax.broadcasted_iota(jnp.int32, (16, TILE), 1)
            ones[slot, r] = jnp.where(idx < cnt, 1.0, 0.0).astype(BF)

    @pl.when(g == 0)
    def _():
        for a in range(arrays):
            slot = sc[a]

            @pl.when(slot >= 0)
            def _():
                pltpu.make_async_copy(kv[a], buf.at[slot], sems.at[slot]).start()

        wait(0)

    goff = pl.multiple_of(g * HEAD_SIZE, HEAD_SIZE)

    def keys(slot, r):
        return buf[slot, r, 0, :, pl.ds(goff, HEAD_SIZE)]

    def vals(slot, r):
        return jnp.concatenate([buf[slot, r, 1, pl.ds(goff, HEAD_SIZE), :], ones[slot, r]], axis=0)

    def chain(h, t, slot, first_tile, last_tile, mode, first):
        c = h * tiles + t
        q = q_ref[t * TILE : (t + 1) * TILE, h * HEAD_SIZE : (h + 1) * HEAD_SIZE]
        rng = range(first_tile, last_tile)
        s = [_dot_nt(keys(slot, r), q) for r in rng]
        if mode == "own":
            ks = lax.broadcasted_iota(jnp.int32, (TILE, TILE), 0)
            qs = lax.broadcasted_iota(jnp.int32, (TILE, TILE), 1)
            s[-1] = jnp.where(ks <= qs, s[-1], NEG)
        elif mode == "edge":
            ks = lax.broadcasted_iota(jnp.int32, (TILE, TILE), 0)
            qs = lax.broadcasted_iota(jnp.int32, (TILE, TILE), 1)
            cnt = sc[cbase + slot]
            for n, r in enumerate(rng):
                ok = ks < cnt - r * TILE
                if r == t:
                    ok = ok & (ks > qs)
                s[n] = jnp.where(ok, s[n], NEG)
        s = jnp.concatenate(s, axis=0) if len(s) > 1 else s[0]
        m_new = jnp.max(s, axis=0, keepdims=True)
        if not first:
            m_old = m_ref[c]
            m_new = jnp.maximum(m_old, m_new)
        p = jnp.exp2(s - m_new).astype(BF)
        v = [vals(slot, r) for r in rng]
        v = jnp.concatenate(v, axis=1) if len(v) > 1 else v[0]
        o = _dot(v, p)
        if not first:
            o = acc_ref[c] * jnp.exp2(m_old - m_new) + o
        m_ref[c] = m_new
        acc_ref[c] = o

    for h in range(heads):
        for t in range(tiles):
            chain(h, t, 0, 0, t + 1, "own", True)

    def body(n, carry):
        slot = n + 2

        @pl.when(g == 0)
        def _():
            wait(slot)

        for h in range(heads):
            for t in range(tiles):
                chain(h, t, slot, 0, tiles, "full", False)
        return carry

    lax.fori_loop(0, interior, body, 0)

    @pl.when(has_edge > 0)
    def _():
        @pl.when(g == 0)
        def _():
            wait(1)

        for h in range(heads):
            for t in range(tiles):
                chain(h, t, 1, t, tiles, "edge", False)

    for h in range(heads):
        for t in range(tiles):
            c = h * tiles + t
            o = acc_ref[c, 0:HEAD_SIZE, :] * (1.0 / acc_ref[c, HEAD_SIZE : HEAD_SIZE + 1, :])
            out[t * TILE : (t + 1) * TILE, h * HEAD_SIZE : (h + 1) * HEAD_SIZE] = jnp.transpose(
                o
            ).astype(BF)


def attention(scal, q, blocks, groups):
    rows, width = q.shape
    arrays = len(blocks)
    gw = width // groups
    heads = gw // HEAD_SIZE
    tiles = rows // TILE
    slots = WINDOW // rows + 1
    shape = blocks[0].shape
    spec = pl.BlockSpec
    return pl.pallas_call(
        functools.partial(_attn_kernel, arrays=arrays, heads=heads, tiles=tiles),
        grid_spec=pltpu.PrefetchScalarGridSpec(
            num_scalar_prefetch=1,
            grid=(groups,),
            in_specs=[spec((rows, gw), lambda g, sc: (0, g))]
            + [spec(memory_space=pltpu.HBM)] * arrays,
            out_specs=spec((rows, gw), lambda g, sc: (0, g)),
            scratch_shapes=[
                pltpu.VMEM((slots,) + shape, BF),
                pltpu.VMEM((slots, tiles, 16, TILE), BF),
                pltpu.VMEM((heads * tiles, 1, TILE), F32),
                pltpu.VMEM((heads * tiles, HEAD_SIZE + 16, TILE), F32),
                pltpu.SemaphoreType.DMA((slots,)),
            ],
        ),
        out_shape=jax.ShapeDtypeStruct((rows, width), BF),
        compiler_params=pltpu.CompilerParams(dimension_semantics=("arbitrary",)),
        name="window_attention",
    )(scal, q, *blocks)


def _out_full_kernel(sc, a_own, a_oth0, a_oth1, w_own, w_r, w_s, r_own, r_oth, o_own, o_oth, *, half):
    j = pl.program_id(0)
    p0 = _dot(a_own[...], w_own[...]).astype(BF).astype(F32)
    p1 = (_dot(a_oth0[...], w_r[...]) + _dot(a_oth1[...], w_s[...])).astype(BF).astype(F32)
    p = p0 + p1

    @pl.when(j < half)
    def _():
        o_own[...] = (r_own[...].astype(F32) + p).astype(BF)

    @pl.when(j >= half)
    def _():
        o_oth[...] = (r_oth[...].astype(F32) + p).astype(BF)


def out_full(layer, scal, a_own, a_oth, w_out, w_r, w_s, r_own, r_oth):
    rows, half = r_own.shape
    inner = a_own.shape[1]
    cols = 256
    nh = half // cols
    spec = pl.BlockSpec

    def col(j, sc):
        return jnp.where(j < nh, sc[0], 1 - sc[0]) * nh + j % nh

    first = spec((rows, cols), lambda j, sc: (0, jnp.minimum(j, nh - 1)))
    second = spec((rows, cols), lambda j, sc: (0, jnp.maximum(j - nh, 0)))
    return pl.pallas_call(
        functools.partial(_out_full_kernel, half=nh),
        grid_spec=pltpu.PrefetchScalarGridSpec(
            num_scalar_prefetch=1,
            grid=(2 * nh,),
            in_specs=[
                spec((rows, inner), lambda j, sc: (0, 0)),
                spec((rows, inner // 2), lambda j, sc: (0, sc[2])),
                spec((rows, inner // 2), lambda j, sc: (0, 1 - sc[2])),
                spec((None, inner, cols), lambda j, sc: (layer, 0, col(j, sc))),
                spec((inner // 2, cols), lambda j, sc: (0, col(j, sc))),
                spec((inner // 2, cols), lambda j, sc: (0, col(j, sc))),
                first,
                second,
            ],
            out_specs=[first, second],
        ),
        out_shape=[jax.ShapeDtypeStruct((rows, half), BF)] * 2,
        compiler_params=pltpu.CompilerParams(dimension_semantics=("arbitrary",)),
        name="out_full",
    )(scal, a_own, a_oth, a_oth, w_out, w_r, w_s, r_own, r_oth)


def _out_send_kernel(sc, a, w, o):
    o[...] = _dot(a[...], w[...]).astype(BF)


def _out_keep_kernel(sc, a, w, res, o):
    o[...] = res[...].astype(F32) + _dot(a[...], w[...]).astype(BF).astype(F32)


def out_half(layer, scal, a, w_out, res):
    rows, inner = a.shape
    half = w_out.shape[2] // 2
    cols = 256
    nh = half // cols
    spec = pl.BlockSpec
    block = spec((rows, cols), lambda j, sc: (0, j))
    keep = res is not None

    def col(j, sc):
        return (sc[0] if keep else 1 - sc[0]) * nh + j

    return pl.pallas_call(
        _out_keep_kernel if keep else _out_send_kernel,
        grid_spec=pltpu.PrefetchScalarGridSpec(
            num_scalar_prefetch=1,
            grid=(nh,),
            in_specs=[
                spec((rows, inner), lambda j, sc: (0, 0)),
                spec((None, inner, cols), lambda j, sc: (layer, 0, col(j, sc))),
            ]
            + ([block] if keep else []),
            out_specs=block,
        ),
        out_shape=jax.ShapeDtypeStruct((rows, half), F32 if keep else BF),
        compiler_params=pltpu.CompilerParams(dimension_semantics=("arbitrary",)),
        name="out_keep" if keep else "out_send",
    )(scal, a, w_out, *([res] if keep else []))


def per_device(tokens, norm_gain, w_query, w_key, w_value, w_out, counts):
    rows = tokens.shape[0]
    layers = w_query.shape[0]
    groups = w_key.shape[2] // HEAD_SIZE
    n = lax.axis_size("seq")
    i = lax.axis_index("seq")
    hd = lax.axis_index("head")
    span = WINDOW // rows
    assert span == 8 and n % 4 == 0 and lax.axis_size("head") == 2

    def swap_head(x):
        return lax.ppermute(x, "head", [(0, 1), (1, 0)])

    def move(x, pairs):
        return lax.ppermute(x, "seq", pairs)

    every = range(n)
    up4 = [(s, s + 4) for s in range(n - 4)]
    low_to_high = [(s, s + 2) for s in every if s % 4 < 2]
    high_to_low = [(s, s - 2) for s in every if s % 4 >= 2]
    even_to_odd = [(s, s + 1) for s in every if s % 2 == 0]
    odd_to_even = [(s, s - 1) for s in every if s % 2 == 1]
    pair = even_to_odd + odd_to_even

    own, oth = tokens, swap_head(tokens)
    core = i % 2
    inner = w_out.shape[1]
    w_piece = lax.dynamic_slice_in_dim(w_out[0], core * (inner // 2), inner // 2, 0)
    w_r = swap_head(w_piece)
    w_s = move(w_r, pair)

    freq = jnp.power(F32(rope_base), -2.0 * jnp.arange(HEAD_SIZE // 2, dtype=F32) / HEAD_SIZE)
    pos = (i * rows + jnp.arange(rows, dtype=jnp.int32)).astype(F32)
    angle = pos[:, None] * freq[None, :]
    c, s = jnp.cos(angle), jnp.sin(angle)
    cos = jnp.concatenate([c, c], axis=1)
    sin = jnp.concatenate([-s, s], axis=1)

    low = (i & 2) == 0
    even = (i & 1) == 0
    none = jnp.int32(-1)
    ids = jnp.stack(
        [
            i,
            i - 8,
            jnp.where(even, none, i - 1),
            i - 4,
            (i ^ 1) - 4,
            jnp.where(low, none, i - 2),
            jnp.where(low, none, (i ^ 1) - 2),
            (i ^ 2) - 4,
            (i ^ 3) - 4,
            jnp.where(even, i - 7, none),
            jnp.where(low, i - 6, none),
            jnp.where(low, (i ^ 3) - 8, none),
        ]
    )
    inside = (ids >= jnp.maximum(i - 7, 0)) & (ids < i)
    rank = jnp.cumsum(inside.astype(jnp.int32)) - inside.astype(jnp.int32)
    slot = jnp.where(inside, rank + 2, -1)
    slot = slot.at[0].set(0).at[1].set(jnp.where(i >= 8, 1, -1))
    hit = slot[None, :] == jnp.arange(span + 1)[:, None]
    block_of = jnp.sum(jnp.where(hit, ids[None, :], 0), axis=1)
    cnt = jnp.sum(
        jnp.where(block_of[:, None] == jnp.arange(counts.shape[0])[None, :], counts[None, :], 0),
        axis=1,
    )
    scal_attn = jnp.concatenate(
        [slot, jnp.sum(inside.astype(jnp.int32))[None], (i >= 8).astype(jnp.int32)[None], cnt]
    ).astype(jnp.int32)
    scal = jnp.stack([hd, cnt[0], core]).astype(jnp.int32)

    for layer in range(layers):
        pay, na, nb = kv_project(layer, scal, own, oth, norm_gain, w_key, w_value, cos, sin)
        r1 = move(pay, up4)
        y0 = move(pay, low_to_high)
        p1 = move(pay, even_to_odd)
        r2 = move(r1, up4)
        y1 = move(r1, low_to_high + high_to_low)
        s1 = move(r1, pair)
        sy0 = move(y0, pair)
        y2 = move(r2, high_to_low)
        sy1 = move(y1, pair)
        s2 = move(r2, odd_to_even)
        sy2 = move(y2, pair)
        q = q_project(layer, scal, na, nb, w_query, cos, sin)
        blocks = [pay, r2, p1, r1, s1, y0, sy0, y1, sy1, s2, y2, sy2]
        att = attention(scal_attn, q, blocks, groups)
        if layer < layers - 1:
            att_oth = swap_head(att)
            own, oth = out_full(layer, scal, att, att_oth, w_out, w_r, w_s, own, oth)
        else:
            sent = swap_head(out_half(layer, scal, att, w_out, None))
            kept = out_half(layer, scal, att, w_out, own)
            return (kept + sent.astype(F32)).astype(BF)


def solution(mesh):
    return jax.shard_map(
        per_device,
        mesh=mesh,
        in_specs=(
            P("seq", "head"),
            P(),
            P(None, None, "head"),
            P(None, None, "head"),
            P(None, None, "head"),
            P(None, "head", None),
            P(),
        ),
        out_specs=P("seq", "head"),
        check_vma=False,
    )
```

```python
import functools
import math

import jax
import jax.numpy as jnp
from jax import lax
from jax.experimental import pallas as pl
from jax.experimental.pallas import tpu as pltpu
from jax.sharding import PartitionSpec as P

HEAD_SIZE = 128
WINDOW = 4096
norm_epsilon = 1e-05
rope_base = 10000.0
NEG = -1e30
TILE = 256
BF = jnp.bfloat16
F32 = jnp.float32


def _dot(a, b):
    return jnp.dot(a, b, preferred_element_type=F32)


def _dot_nt(a, b):
    return lax.dot_general(a, b, (((1,), (1,)), ((), ())), preferred_element_type=F32)


def _cost(us):
    return pl.CostEstimate(flops=int(us * 4.5e8), bytes_accessed=1 << 20, transcendentals=0)


def _params():
    return pltpu.CompilerParams(dimension_semantics=("arbitrary",), vmem_limit_bytes=24 << 20)


def _kv_kernel(
    sc, own, oth, g_own, g_oth, wk_own, wk_oth, wv_own, wv_oth, cos, sin, keep, send, n_own, n_oth, row0
):
    step = pl.program_id(0)
    a = own[...].astype(F32)
    b = oth[...].astype(F32)
    width = a.shape[1] + b.shape[1]
    total = jnp.sum(a * a, axis=1, keepdims=True) + jnp.sum(b * b, axis=1, keepdims=True)
    r = lax.rsqrt(total * (1.0 / width) + norm_epsilon)
    na = (a * r * g_own[...]).astype(BF)
    nb = (b * r * g_oth[...]).astype(BF)
    n_own[...] = na
    n_oth[...] = nb
    k = _dot(na, wk_own[...]) + _dot(nb, wk_oth[...])
    v = _dot(na, wv_own[...]) + _dot(nb, wv_oth[...])
    c = cos[...]
    s = sin[...]
    rows = a.shape[0]
    d = HEAD_SIZE
    first = sc[2] == 0
    valid = (step * rows + lax.broadcasted_iota(jnp.int32, (rows, d), 0)) < sc[1]
    ks, vs = [], []
    for h in range(2):
        x = k[:, h * d : (h + 1) * d]
        ks.append(x * c + pltpu.roll(x, d // 2, 1) * s)
        vs.append(v[:, h * d : (h + 1) * d])

    @pl.when(step == 0)
    def _():
        row0[...] = jnp.concatenate([ks[0][0:8, :], ks[1][0:8, :]], axis=1)

    outs = []
    for h in range(2):
        kk = jnp.where(valid, ks[h], row0[0:1, h * d : (h + 1) * d]).astype(BF)
        vv = jnp.transpose(jnp.where(valid, vs[h], 0.0)).astype(BF)
        outs.append((kk, vv))
    for ref, (p, q) in ((keep, outs), (send, outs[::-1])):
        ref[0] = jnp.where(first, p[0], q[0])
        vv = jnp.where(first, p[1], q[1])
        for z in range(rows // d):
            ref[1, z * d : (z + 1) * d, :] = vv[:, z * d : (z + 1) * d]


def kv_project(layer, scal, own, oth, gain, wk, wv, cos, sin):
    rows, half = own.shape
    width = wk.shape[2]
    spec = pl.BlockSpec
    half_rows = spec((TILE, half), lambda r, sc: (r, 0))
    table = spec((TILE, HEAD_SIZE), lambda r, sc: (r, 0))
    w_own = spec((None, half, width), lambda r, sc: (layer, sc[0], 0))
    w_oth = spec((None, half, width), lambda r, sc: (layer, 1 - sc[0], 0))
    gain4 = gain.reshape(gain.shape[0], 2, 1, half)
    ga = spec((None, None, 1, half), lambda r, sc: (layer, sc[0], 0, 0))
    gb = spec((None, None, 1, half), lambda r, sc: (layer, 1 - sc[0], 0, 0))
    steps = rows // TILE
    pay = spec((None, 2, TILE, HEAD_SIZE), lambda r, sc: (r, 0, 0, 0))
    pay_shape = jax.ShapeDtypeStruct((steps, 2, TILE, HEAD_SIZE), BF)
    return pl.pallas_call(
        _kv_kernel,
        grid_spec=pltpu.PrefetchScalarGridSpec(
            num_scalar_prefetch=1,
            grid=(steps,),
            in_specs=[half_rows, half_rows, ga, gb, w_own, w_oth, w_own, w_oth, table, table],
            out_specs=[pay, pay, half_rows, half_rows],
            scratch_shapes=[pltpu.VMEM((8, width), F32)],
        ),
        out_shape=[
            pay_shape,
            pay_shape,
            jax.ShapeDtypeStruct((rows, half), BF),
            jax.ShapeDtypeStruct((rows, half), BF),
        ],
        compiler_params=_params(),
        cost_estimate=_cost(5),
        name="kv_project",
    )(scal, own, oth, gain4, gain4, wk, wk, wv, wv, cos, sin)


def _q_kernel(sc, na, nb, w_own, w_oth, cos, sin, keep, send):
    j = pl.program_id(0)
    q = _dot(na[...], w_own[...]) + _dot(nb[...], w_oth[...])
    c = cos[...]
    s = sin[...]
    factor = math.log2(math.e) / math.sqrt(HEAD_SIZE)

    def write(out):
        for h in range(q.shape[1] // HEAD_SIZE):
            x = q[:, h * HEAD_SIZE : (h + 1) * HEAD_SIZE]
            y = (x * c + pltpu.roll(x, HEAD_SIZE // 2, 1) * s) * factor
            out[:, h * HEAD_SIZE : (h + 1) * HEAD_SIZE] = y.astype(BF)

    @pl.when(j == 0)
    def _():
        write(send)

    @pl.when(j == 1)
    def _():
        write(keep)


def q_project(layer, scal, na, nb, wq, cos, sin):
    rows, half = na.shape
    cols = wq.shape[2] // 2
    spec = pl.BlockSpec
    full = spec((rows, half), lambda j, sc: (0, 0))
    table = spec((rows, HEAD_SIZE), lambda j, sc: (0, 0))

    def group(j, sc):
        return jnp.where(j == 0, 1 - sc[2], sc[2])

    out = spec((rows, cols), lambda j, sc: (0, 0))
    return pl.pallas_call(
        _q_kernel,
        grid_spec=pltpu.PrefetchScalarGridSpec(
            num_scalar_prefetch=1,
            grid=(2,),
            in_specs=[
                full,
                full,
                spec((None, half, cols), lambda j, sc: (layer, sc[0], group(j, sc))),
                spec((None, half, cols), lambda j, sc: (layer, 1 - sc[0], group(j, sc))),
                table,
                table,
            ],
            out_specs=[out, out],
        ),
        out_shape=[jax.ShapeDtypeStruct((rows, cols), BF)] * 2,
        compiler_params=_params(),
        cost_estimate=_cost(6),
        name="q_project",
    )(scal, na, nb, wq, wq, cos, sin)


SAFE = 99.0


def _attn_kernel(sc, q_self, q_part, *refs, kinds, heads, tiles, first, final):
    kv = refs[: len(kinds)]
    rest = list(refs[len(kinds) :])
    km, qs = rest.pop(), rest.pop()
    m_in, a_in, n_in = (None,) * 3 if first else (rest.pop(0), rest.pop(0), rest.pop(0))
    if final:
        o_self, o_part, m_out, a_out = rest
        n_out = None
    else:
        m_out, a_out, n_out = rest
    step = pl.program_id(0)
    b = step // tiles
    t = step % tiles
    parity = sc[2]
    odd_query = b != parity
    d = HEAD_SIZE

    @pl.when(step == 0)
    def _():
        for n in range(len(kinds)):
            top = None
            for z in range(2):
                for r in range(tiles):
                    k = kv[n][z, r, 0].astype(F32)
                    sq = jnp.sum(k * k, axis=1, keepdims=True)
                    top = sq if top is None else jnp.maximum(top, sq)
            km[n] = jnp.max(top)

    def query(h):
        lanes = pl.ds(pl.multiple_of(h * d, d), d)
        return jnp.where(b == 0, q_self[:, lanes], q_part[:, lanes])

    if first:
        top = None
        for h in range(heads):
            q = query(h).astype(F32)
            sq = jnp.sum(q * q, axis=1, keepdims=True)
            top = sq if top is None else jnp.maximum(top, sq)
        qs[0] = jnp.max(top)
    else:
        m_out[...] = m_in[...]
        a_out[...] = a_in[...]
        qs[0] = jnp.max(n_in[0:1, :])

    def keys(ref, blocks, rng):
        return [ref[z, r, 0] for z in blocks for r in rng]

    def vals(ref, base, blocks, rng):
        out = []
        for z in blocks:
            cnt = sc[base + z]
            for r in rng:
                x = ref[z, r, 1]
                vt = jnp.concatenate([x[y * d : (y + 1) * d] for y in range(TILE // d)], axis=1)
                idx = r * TILE + lax.broadcasted_iota(jnp.int32, (16, TILE), 1)
                one = jnp.where(idx < cnt, 1.0, 0.0).astype(BF)
                out.append(jnp.concatenate([vt, one], axis=0))
        return jnp.concatenate(out, axis=1) if len(out) > 1 else out[0]

    def fast(k, v, masks, fresh):
        for h in range(heads):
            q = query(h)
            p = [jnp.exp2(_dot_nt(x, q)) for x in k]
            p = [x if ok is None else jnp.where(ok, x, 0.0) for x, ok in zip(p, masks)]
            p = [x.astype(BF) for x in p]
            p = jnp.concatenate(p, axis=0) if len(p) > 1 else p[0]
            o = _dot(v, p)
            if fresh:
                m_out[h] = jnp.zeros(m_out.shape[1:], F32)
                a_out[h] = o
            else:
                a_out[h] = a_out[h] + o

    def slow(k, v, masks, fresh):
        qs[0] = jnp.float32(1e30)

        def one_head(h, carry):
            q = query(h)
            s = [_dot_nt(x, q) for x in k]
            s = [x if ok is None else jnp.where(ok, x, NEG) for x, ok in zip(s, masks)]
            s = jnp.concatenate(s, axis=0) if len(s) > 1 else s[0]
            m_new = jnp.max(s, axis=0, keepdims=True)
            if not fresh:
                m_old = m_out[h]
                m_new = jnp.maximum(m_old, m_new)
            o = _dot(v, jnp.exp2(s - m_new).astype(BF))
            if not fresh:
                o = a_out[h] * jnp.exp2(m_old - m_new) + o
            m_out[h] = m_new
            a_out[h] = o
            return carry

        lax.fori_loop(0, heads, one_head, 0)

    ks = lax.broadcasted_iota(jnp.int32, (TILE, TILE), 0)
    qi = lax.broadcasted_iota(jnp.int32, (TILE, TILE), 1)
    flag = 3
    base = 3 + len(kinds)

    def run(n, active, make, fresh):
        safe = qs[0] * km[n] <= SAFE * SAFE

        @pl.when(active & safe)
        def _():
            fast(*make(), fresh)

        @pl.when(active & jnp.logical_not(safe))
        def _():
            slow(*make(), fresh)

    for n, kind in enumerate(kinds):
        ref = kv[n]
        cb = base + 2 * n
        rng = range(tiles)
        some = sc[flag + n] > 0
        if kind == "own":
            for tt in range(tiles):

                def diag(tt=tt):
                    up = range(tt + 1)
                    return keys(ref, [b], up), vals(ref, cb, [b], up), [None] * tt + [ks <= qi]

                run(n, t == tt, diag, True)

            def before():
                return keys(ref, [parity], rng), vals(ref, cb, [parity], rng), [None] * tiles

            run(n, odd_query, before, False)

        elif kind == "full":

            def both():
                z = [0, 1]
                return keys(ref, z, rng), vals(ref, cb, z, rng), [None] * (2 * tiles)

            run(n, some, both, False)

        else:

            def after():
                z = [1 - parity]
                return keys(ref, z, rng), vals(ref, cb, z, rng), [None] * tiles

            run(n, some & jnp.logical_not(odd_query), after, False)

            for tt in range(tiles):

                def edge(tt=tt):
                    up = range(tt, tiles)
                    cnt = sc[cb + b]
                    masks = [
                        (ks < cnt - r * TILE) & (ks > qi) if r == tt else ks < cnt - r * TILE
                        for r in up
                    ]
                    return keys(ref, [b], up), vals(ref, cb, [b], up), masks

                run(n, some & (t == tt), edge, False)

    if final:
        outs = []
        for h in range(heads):
            o = a_out[h, 0:d, :] * (1.0 / a_out[h, d : d + 1, :])
            outs.append(jnp.transpose(o).astype(BF))
        o = jnp.concatenate(outs, axis=1)

        @pl.when(b == 0)
        def _():
            o_self[...] = o

        @pl.when(b == 1)
        def _():
            o_part[...] = o

    else:
        n_out[...] = jnp.full(n_out.shape, qs[0], F32)


def attention(scal, q_self, q_part, parts, state, final, us):
    rows, width = q_self.shape
    heads = width // HEAD_SIZE
    tiles = rows // TILE
    steps = 2 * tiles
    kinds = tuple(kind for kind, _, _, _ in parts)
    blocks = [x for _, x, _, _ in parts]
    flags = [jnp.asarray(f, jnp.int32)[None] for _, _, f, _ in parts]
    counts = [jnp.asarray(c, jnp.int32) for _, _, _, c in parts]
    sc = jnp.concatenate([scal] + flags + counts)
    spec = pl.BlockSpec
    q_spec = spec((TILE, width), lambda s, sc: (s % tiles, 0))
    shape = blocks[0].shape
    whole = spec(shape, lambda s, sc: (0,) * len(shape))
    m_spec = spec((None, heads, 1, TILE), lambda s, sc: (s, 0, 0, 0))
    a_spec = spec((None, heads, HEAD_SIZE + 16, TILE), lambda s, sc: (s, 0, 0, 0))
    n_spec = spec((None, 8, HEAD_SIZE), lambda s, sc: (s, 0, 0))
    n_shape = jax.ShapeDtypeStruct((steps, 8, HEAD_SIZE), F32)
    m_shape = jax.ShapeDtypeStruct((steps, heads, 1, TILE), F32)
    a_shape = jax.ShapeDtypeStruct((steps, heads, HEAD_SIZE + 16, TILE), F32)
    first = state is None
    in_specs = [q_spec, q_spec] + [whole] * len(blocks) + ([] if first else [m_spec, a_spec, n_spec])
    args = [sc, q_self, q_part] + blocks + ([] if first else list(state))
    if final:
        o1 = spec((TILE, width), lambda s, sc: (jnp.minimum(s, tiles - 1), 0))
        o2 = spec((TILE, width), lambda s, sc: (jnp.maximum(s - tiles, 0), 0))
        out_specs = [o1, o2]
        out_shape = [jax.ShapeDtypeStruct((rows, width), BF)] * 2
        scratch = [
            pltpu.VMEM((heads, 1, TILE), F32),
            pltpu.VMEM((heads, HEAD_SIZE + 16, TILE), F32),
        ]
    else:
        out_specs = [m_spec, a_spec, n_spec]
        out_shape = [m_shape, a_shape, n_shape]
        scratch = []
    return pl.pallas_call(
        functools.partial(
            _attn_kernel, kinds=kinds, heads=heads, tiles=tiles, first=first, final=final
        ),
        grid_spec=pltpu.PrefetchScalarGridSpec(
            num_scalar_prefetch=1,
            grid=(steps,),
            in_specs=in_specs,
            out_specs=out_specs,
            scratch_shapes=scratch
            + [pltpu.SMEM((1,), F32), pltpu.SMEM((len(blocks),), F32)],
        ),
        out_shape=out_shape,
        compiler_params=_params(),
        cost_estimate=_cost(us),
        name="attention_" + "_".join(kinds),
    )(*args)


def _out_full_kernel(sc, a0, a1, b0, b1, w0, w1, w_r, w_s, r_own, r_oth, o_own, o_oth, *, half):
    j = pl.program_id(0)
    p0 = (_dot(a0[...], w0[...]) + _dot(a1[...], w1[...])).astype(BF).astype(F32)
    p1 = (_dot(b0[...], w_r[...]) + _dot(b1[...], w_s[...])).astype(BF).astype(F32)
    p = p0 + p1

    @pl.when(j < half)
    def _():
        o_own[...] = (r_own[...].astype(F32) + p).astype(BF)

    @pl.when(j >= half)
    def _():
        o_oth[...] = (r_oth[...].astype(F32) + p).astype(BF)


def out_full(layer, scal, pieces, w_out, w_r, w_s, r_own, r_oth):
    rows, half = r_own.shape
    inner = pieces[0].shape[1]
    cols = 512
    nh = half // cols
    spec = pl.BlockSpec

    def col(j, sc):
        return jnp.where(j < nh, sc[0], 1 - sc[0]) * nh + j % nh

    first = spec((rows, cols), lambda j, sc: (0, jnp.minimum(j, nh - 1)))
    second = spec((rows, cols), lambda j, sc: (0, jnp.maximum(j - nh, 0)))
    a_spec = spec((rows, inner), lambda j, sc: (0, 0))
    w_spec = spec((inner, cols), lambda j, sc: (0, col(j, sc)))
    return pl.pallas_call(
        functools.partial(_out_full_kernel, half=nh),
        grid_spec=pltpu.PrefetchScalarGridSpec(
            num_scalar_prefetch=1,
            grid=(2 * nh,),
            in_specs=[a_spec] * 4
            + [
                spec((None, inner, cols), lambda j, sc: (layer, sc[2], col(j, sc))),
                spec((None, inner, cols), lambda j, sc: (layer, 1 - sc[2], col(j, sc))),
                w_spec,
                w_spec,
                first,
                second,
            ],
            out_specs=[first, second],
        ),
        out_shape=[jax.ShapeDtypeStruct((rows, half), BF)] * 2,
        compiler_params=_params(),
        cost_estimate=_cost(8),
        name="out_full",
    )(scal, *pieces, w_out, w_out, w_r, w_s, r_own, r_oth)


def _out_send_kernel(sc, a0, a1, w0, w1, o):
    o[...] = (_dot(a0[...], w0[...]) + _dot(a1[...], w1[...])).astype(BF)


def _out_keep_kernel(sc, a0, a1, w0, w1, res, o):
    p = (_dot(a0[...], w0[...]) + _dot(a1[...], w1[...])).astype(BF)
    o[...] = res[...].astype(F32) + p.astype(F32)


def out_half(layer, scal, pieces, w_out, res):
    rows, inner = pieces[0].shape
    half = w_out.shape[2] // 2
    cols = 512
    nh = half // cols
    spec = pl.BlockSpec
    block = spec((rows, cols), lambda j, sc: (0, j))
    keep = res is not None

    def col(j, sc):
        return (sc[0] if keep else 1 - sc[0]) * nh + j

    a_spec = spec((rows, inner), lambda j, sc: (0, 0))
    return pl.pallas_call(
        _out_keep_kernel if keep else _out_send_kernel,
        grid_spec=pltpu.PrefetchScalarGridSpec(
            num_scalar_prefetch=1,
            grid=(nh,),
            in_specs=[
                a_spec,
                a_spec,
                spec((None, inner, cols), lambda j, sc: (layer, sc[2], col(j, sc))),
                spec((None, inner, cols), lambda j, sc: (layer, 1 - sc[2], col(j, sc))),
            ]
            + ([block] if keep else []),
            out_specs=block,
        ),
        out_shape=jax.ShapeDtypeStruct((rows, half), F32 if keep else BF),
        compiler_params=_params(),
        cost_estimate=_cost(4),
        name="out_keep" if keep else "out_send",
    )(scal, *pieces, w_out, w_out, *([res] if keep else []))


def per_device(tokens, norm_gain, w_query, w_key, w_value, w_out, counts):
    rows = tokens.shape[0]
    layers = w_query.shape[0]
    n = lax.axis_size("seq")
    i = lax.axis_index("seq")
    hd = lax.axis_index("head")
    assert WINDOW == 8 * rows and n % 4 == 0 and lax.axis_size("head") == 2
    assert w_key.shape[2] == 2 * HEAD_SIZE

    def swap_head(x):
        return lax.ppermute(x, "head", [(0, 1), (1, 0)])

    def swap_core(x):
        return lax.ppermute(x, "seq", [(s, s ^ 1) for s in range(n)])

    def swap_pair(x):
        return lax.ppermute(x, "seq", [(s, s ^ 2) for s in range(n)])

    def up(x):
        return lax.ppermute(x, "seq", [(s, (s + 4) % n) for s in range(n)])

    own, oth = tokens, swap_head(tokens)
    core = i % 2
    inner = w_out.shape[1]
    w_piece = lax.dynamic_slice_in_dim(w_out, core * (inner // 2), inner // 2, 1)[0]
    w_r = swap_head(w_piece)
    w_s = swap_core(w_r)

    freq = jnp.power(F32(rope_base), -2.0 * jnp.arange(HEAD_SIZE // 2, dtype=F32) / HEAD_SIZE)
    pos = (i * rows + jnp.arange(rows, dtype=jnp.int32)).astype(F32)
    angle = pos[:, None] * freq[None, :]
    c, s = jnp.cos(angle), jnp.sin(angle)
    cos = jnp.concatenate([c, c], axis=1)
    sin = jnp.concatenate([-s, s], axis=1)

    def count_of(block):
        ids = jnp.stack([block, block ^ 1])
        hit = ids[:, None] == jnp.arange(counts.shape[0])[None, :]
        return jnp.sum(jnp.where(hit, counts[None, :], 0), axis=1)

    high = (i & 2) != 0
    one = i >= 4
    two = i >= 8
    c_own = count_of(i)
    c_r1, c_r2 = count_of(i - 4), count_of(i - 8)
    c_y0, c_y1, c_y2 = count_of(i ^ 2), count_of((i ^ 2) - 4), count_of((i ^ 2) - 8)
    scal = jnp.stack([hd, c_own[0], core]).astype(jnp.int32)

    for layer in range(layers):
        keep, send, na, nb = kv_project(layer, scal, own, oth, norm_gain, w_key, w_value, cos, sin)
        pay = jnp.stack([keep, swap_core(send)])
        r1 = up(pay)
        y0 = swap_pair(pay)
        q_self, q_send = q_project(layer, scal, na, nb, w_query, cos, sin)
        q_part = swap_core(q_send)
        run = functools.partial(attention, scal, q_self, q_part)
        state = run([("own", pay, True, c_own)], None, False, 8)
        r1, state = lax.optimization_barrier((r1, state))
        r2 = up(r1)
        y1 = swap_pair(r1)
        state = run([("full", r1, one, c_r1), ("full", y0, high, c_y0)], state, False, 18)
        r2, state = lax.optimization_barrier((r2, state))
        y2 = swap_pair(r2)
        state = run([("edge", r2, two, c_r2), ("full", y1, one, c_y1)], state, False, 20)
        a_self, a_part = run([("full", y2, two & ~high, c_y2)], state, True, 12)
        x_self = swap_head(a_self) if layer < layers - 1 else None
        a_mine = swap_core(a_part)
        if layer < layers - 1:
            pieces = [a_self, a_mine, x_self, swap_head(a_mine)]
            own, oth = out_full(layer, scal, pieces, w_out, w_r, w_s, own, oth)
        else:
            sent = swap_head(out_half(layer, scal, [a_self, a_mine], w_out, None))
            kept = out_half(layer, scal, [a_self, a_mine], w_out, own)
            return (kept + sent.astype(F32)).astype(BF)


def solution(mesh):
    return jax.shard_map(
        per_device,
        mesh=mesh,
        in_specs=(
            P("seq", "head"),
            P(),
            P(None, None, "head"),
            P(None, None, "head"),
            P(None, None, "head"),
            P(None, "head", None),
            P(),
        ),
        out_specs=P("seq", "head"),
        check_vma=False,
    )
```
